32 devices in a mesh: grp: 2 (over x), slab: 16 (over z, y, core).
Axes of the slice: x: 2, y: 2, z: 4, core: 2. Of those that a mesh axis runs over, the one named last changes fastest.
Arguments:
- sample_xy: float32 [2, 16, 8, 2, 256], P('grp', 'slab'), may hold values from 0 to 384
- sample_dz: float32 [2, 16, 8, 256], P('grp', 'slab'), may hold values from 0 to 1
- sample_values: float32 [2, 16, 8, 2, 256], P('grp', 'slab'), may hold values from -6 to 6
- block_tile: int32 [2, 16, 8], P('grp', 'slab'), may hold values from 0 to 5
- block_count: int32 [2, 16, 8], P('grp', 'slab'), may hold values from 1 to 256
Outputs:
- grid_sum: float32 [384, 96, 2, 384], P('grp', 'slab')
The draws below stay inside these ranges and needn't reach their ends.
Inputs may be any that keep to these rules, and one draw needn't show every extreme that they name: `block_tile`: the base plane of every sample of a block. Slots from block_count on hold values that are not used.
All inputs are finite; a program needn't handle non-finite values.
Results may differ from the reference program's by a relative error of at most 0.0037.
Values sent between devices are 32-bit elements; how exact they have to be, the bound alone decides.
A program may use at most 192 MiB of HBM per device.

```python
import math
import jax
import jax.numpy as jnp
from jax import lax

NX = 384
NY = 384
BLOCK = 256
PLANES = 6
BLOCKS_DEV = 8
NZ = 96
N_GRP = 2
N_SLAB = 16


def place_ends(array, rng, smallest, high):
    shape = array.shape
    index_at = [jax.random.randint(jax.random.fold_in(rng, axis), (), 0, shape[axis]) for axis in range(len(shape))]
    array = array.at[tuple(index_at)].set(smallest)
    longest = shape.index(max(shape))
    index_at[longest] = (index_at[longest] + 1) % shape[longest]
    return array.at[tuple(index_at)].set(high)


def block_scale(key, dims, pieces, smallest, high):
    loudness, own = 1.0, jax.random.fold_in(key, 6)
    for axis_at, parts in pieces:
        draws = jnp.exp(jax.random.uniform(jax.random.fold_in(own, axis_at), (parts,), jnp.float32, smallest / len(pieces), high / len(pieces)))
        loudness = loudness * jnp.repeat(draws, dims[axis_at] // parts).reshape([-1 if axis == axis_at else 1 for axis in range(len(dims))])
    return loudness


def centred(own_key, shape, scale, most, shards=(), kind=jnp.bfloat16):
    array = jax.random.normal(own_key, shape, jnp.float32) * scale
    if len(shards) > 0:
        array = block_scale(own_key, shape, shards, -0.22, 0.18) * array
    return jnp.clip(array, min=-most, max=most).astype(kind)


def setup_inputs(seed: int = 0) -> dict:
    arg_keys = jax.random.split(jax.random.key(seed), 6)
    sample_xy = jnp.clip(384.0 * jax.random.uniform(arg_keys[0], (N_GRP, N_SLAB, BLOCKS_DEV, 2, BLOCK), jnp.float32) ** block_scale(arg_keys[0], (N_GRP, N_SLAB, BLOCKS_DEV, 2, BLOCK), ((0, 2), (1, 16)), -0.2, 0.2), 0.0, 384.0)
    sample_dz = jnp.clip(1.0 * jax.random.uniform(arg_keys[1], (N_GRP, N_SLAB, BLOCKS_DEV, BLOCK), jnp.float32) ** block_scale(arg_keys[1], (N_GRP, N_SLAB, BLOCKS_DEV, BLOCK), ((0, 2), (1, 16)), -0.2, 0.2), 0.0, 1.0)
    sample_values = centred(arg_keys[2], (N_GRP, N_SLAB, BLOCKS_DEV, 2, BLOCK), 1.0, 6.0, ((0, 2), (1, 16)), jnp.float32)
    block_tile = place_ends(jax.random.randint(arg_keys[3], (N_GRP, N_SLAB, BLOCKS_DEV), 0, PLANES), jax.random.fold_in(arg_keys[3], 1), 0, PLANES - 1).astype(jnp.int32)
    block_count = place_ends(jax.random.randint(arg_keys[4], (N_GRP, N_SLAB, BLOCKS_DEV), 1, BLOCK + 1), jax.random.fold_in(arg_keys[4], 1), 1, BLOCK).astype(jnp.int32)
    return dict(sample_xy=sample_xy, sample_dz=sample_dz, sample_values=sample_values, block_tile=block_tile, block_count=block_count)


BETA = math.pi * math.sqrt(19.45)

def kaiser_top():
    half_sq = (0.5 * BETA) ** 2
    term = 1.0
    total = 1.0
    for order in range(1, 32):
        term = term * half_sq / (order * order)
        total = total + term
    return total - 1.0

def bessel_zero(arg):
    half_sq = 0.5 * arg * (0.5 * arg)
    term = jnp.ones_like(arg)
    total = term
    for order in range(1, 32):
        term = term * half_sq / float(order * order)
        total = total + term
    return total

def kaiser(distance):
    inside = jnp.maximum(1.0 - (distance / 3.0) ** 2, 0.0)
    bessel = bessel_zero(BETA * jnp.sqrt(inside))
    return (bessel - 1.0) / kaiser_top()

def reference(sample_xy, sample_dz, sample_values, block_tile, block_count):
    offsets = jnp.arange(6).astype(sample_xy.dtype)
    offsets_int = jnp.arange(6).astype(jnp.int32)
    lane_ids = jnp.arange(BLOCK).astype(jnp.int32)
    index_c = jnp.arange(2).astype(jnp.int32)

    def one_slab(slab_id, grid_sum):
        coords = lax.dynamic_index_in_dim(sample_xy, slab_id, 1, keepdims=False).reshape(-1, 2, BLOCK)
        depths = lax.dynamic_index_in_dim(sample_dz, slab_id, 1, keepdims=False).reshape(-1, BLOCK)
        values = lax.dynamic_index_in_dim(sample_values, slab_id, 1, keepdims=False).reshape(-1, 2, BLOCK)
        tile_ids = lax.dynamic_index_in_dim(block_tile, slab_id, 1, keepdims=False).reshape(-1)
        counts = lax.dynamic_index_in_dim(block_count, slab_id, 1, keepdims=False).reshape(-1)
        pos_x = coords[:, 0]
        pos_y = coords[:, 1]
        cell_x = jnp.floor(pos_x)[..., None] - 2.0 + offsets
        cell_y = jnp.floor(pos_y)[..., None] - 2.0 + offsets
        weight_x = lax.optimization_barrier(kaiser(cell_x - pos_x[..., None]).astype(jnp.bfloat16)).astype(jnp.float32)
        weight_y = kaiser(cell_y - pos_y[..., None])
        weight_z = kaiser(offsets - 2.0 - depths[..., None])
        keep_mask = (lane_ids[None, :] < counts[:, None]).astype(jnp.float32)
        spread_w = (weight_z * keep_mask[..., None])[:, :, :, None, None] * jnp.swapaxes(values, 1, 2)[:, :, None, :, None] * weight_y[:, :, None, None, :]
        spread_w = lax.optimization_barrier(spread_w.astype(jnp.bfloat16)).astype(jnp.float32)
        contrib = weight_x[:, :, :, None, None, None] * spread_w[:, :, None]
        index_x = jnp.mod(cell_x.astype(jnp.int32), NX)
        index_y = jnp.mod(cell_y.astype(jnp.int32), NY)
        index_z = jnp.mod(slab_id * PLANES + tile_ids[:, None] + offsets_int[None, :] - 2, NZ)
        return grid_sum.at[index_x[:, :, :, None, None, None], index_z[:, None, None, :, None, None], index_c[None, None, None, None, :, None], index_y[:, :, None, None, None, :]].add(contrib)
    start_grid = jnp.zeros((NX, NZ, 2, NY), jnp.float32)
    return lax.fori_loop(0, N_SLAB, one_slab, start_grid)
```

```python
import math

import jax
import jax.numpy as jnp
from jax import lax
from jax.experimental import pallas as pl
from jax.experimental.pallas import tpu as pltpu
from jax.sharding import PartitionSpec as P

NX = 384
NY = 384
PLANES = 6
REACH = 3
LEVELS = PLANES + 5
CHUNK = 256
LANES = 128

BETA = math.pi * math.sqrt(19.45)
MESH = pl.DeviceIdType.MESH


def kaiser_coefs():
    half_sq = (0.5 * BETA) ** 2
    term = 1.0
    terms = []
    for order in range(1, 32):
        term = term * half_sq / (order * order)
        terms.append(term)
    top = sum(terms)
    return [value / top for value in terms]


COEFS = kaiser_coefs()


def kaiser(distance):
    scaled = distance * (1.0 / 3.0)
    inside = jnp.maximum(1.0 - scaled * scaled, 0.0)
    total = jnp.full_like(inside, COEFS[-1])
    for coef in COEFS[-2::-1]:
        total = total * inside + coef
    return total * inside


def exchange(groups, slabs, *refs):
    ins, outs = refs[:5], refs[5:10]
    send_sem, recv_sem, self_sem = refs[10:]
    grp = lax.axis_index("grp")
    slab = lax.axis_index("slab")
    partners = []
    for side in range(3):
        for hop in range(groups):
            if side != 1 or hop != 0:
                partners.append(
                    (side, lax.rem(grp + hop, groups), lax.rem(slab + slabs + 1 - side, slabs))
                )
    barrier = pltpu.get_barrier_semaphore()
    for _, g, j in partners:
        pl.semaphore_signal(barrier, inc=1, device_id=(g, j), device_id_type=MESH)
    own = [
        pltpu.make_async_copy(src, dst.at[1, grp], self_sem.at[n])
        for n, (src, dst) in enumerate(zip(ins, outs))
    ]
    for copy in own:
        copy.start()
    pl.semaphore_wait(barrier, len(partners))
    copies = []
    for side, g, j in partners:
        for src, dst in zip(ins, outs):
            copy = pltpu.make_async_remote_copy(
                src_ref=src,
                dst_ref=dst.at[side, grp],
                send_sem=send_sem.at[len(copies)],
                recv_sem=recv_sem.at[len(copies)],
                device_id=(g, j),
                device_id_type=MESH,
            )
            copy.start()
            copies.append(copy)
    for copy in own:
        copy.wait()
    for copy in copies:
        copy.wait()


def widen(cells, weights, repeat, count, first):
    ids = lax.broadcasted_iota(jnp.int32, (count, CHUNK), 0)
    ids = (lax.div(ids, repeat) + first).astype(jnp.float32).astype(jnp.bfloat16)
    wide = jnp.zeros((count, CHUNK), jnp.bfloat16)
    for k in range(6):
        wide = jnp.where(ids == cells[k : k + 1], weights[k : k + 1], wide)
    return wide


def centred_cells(floor, taps_i, period, base, half):
    cell = floor.astype(jnp.int32) - 2 + taps_i
    cell = jnp.where(cell < 0, cell + period, cell)
    cell = jnp.where(cell >= period, cell - period, cell) - (base + half)
    cell = jnp.where((cell >= -half) & (cell < half), cell, 256)
    return cell.astype(jnp.float32).astype(jnp.bfloat16)


def grid_kernel(
    groups, rows, xy, dz, val, tile, cnt, out, comp, acc, wide_x, wide_y, rowsc, stage, start, cursor, sems
):
    blocks = xy.shape[2]
    total_blocks = 3 * groups * blocks
    row_base = lax.axis_index("grp") * rows

    for level in range(LEVELS + 1):
        start[level] = 0
    comp[...] = jnp.zeros_like(comp)

    def where_is(at):
        side = lax.div(at, groups * blocks)
        rest = lax.rem(at, groups * blocks)
        g = lax.div(rest, blocks)
        b = lax.rem(rest, blocks)
        level = tile[side, g, 0, b] + PLANES * (side - 1) + REACH
        return side, g, b, level

    def count(at, carry):
        side, g, b, level = where_is(at)

        @pl.when((level >= 0) & (level < LEVELS))
        def _():
            start[level + 1] = start[level + 1] + cnt[side, g, 0, b]

        return carry

    lax.fori_loop(0, total_blocks, count, 0)
    cursor[0] = 0
    for level in range(1, LEVELS + 1):
        start[level] = start[level] + start[level - 1]
        cursor[level] = start[level]

    lane = lax.broadcasted_iota(jnp.int32, (8, LANES), 1)

    def place(at, carry):
        side, g, b, level = where_is(at)

        @pl.when((level >= 0) & (level < LEVELS))
        def _():
            used = cnt[side, g, 0, b]
            to = cursor[level]
            cursor[level] = to + used
            shift = lax.rem(to, LANES)
            base = pl.multiple_of(to - shift, LANES)
            coords = xy[side, g, b]
            values = val[side, g, b]
            depth = dz[side, g, pl.ds(b, 1), :]
            plane = jnp.full_like(depth, level - REACH)
            packed = jnp.concatenate(
                [coords, values, depth, plane, jnp.zeros_like(coords)], axis=0
            )
            pieces = [
                pltpu.roll(packed[:, p * LANES : (p + 1) * LANES], shift, axis=1)
                for p in range(packed.shape[1] // LANES)
            ]
            for p in range(len(pieces) + 1):
                before = pieces[max(p - 1, 0)]
                after = pieces[min(p, len(pieces) - 1)]
                merged = jnp.where(lane < shift, before, after)
                slot = lane + (p * LANES - shift)
                at_lanes = pl.ds(base + p * LANES, LANES)
                comp[:, at_lanes] = jnp.where(
                    (slot >= 0) & (slot < used), merged, comp[:, at_lanes]
                )

        return carry

    lax.fori_loop(0, total_blocks, place, 0)
    acc[...] = jnp.zeros_like(acc)

    taps_i = lax.broadcasted_iota(jnp.int32, (8, CHUNK), 0)
    taps = taps_i.astype(jnp.float32)
    odd = (lax.broadcasted_iota(jnp.int32, (16, CHUNK), 0) & 1) == 1

    def one_chunk(i, carry):
        first = i * CHUNK
        data = comp[:, pl.ds(pl.multiple_of(first, CHUNK), CHUNK)]
        pos_x, pos_y = data[0:1], data[1:2]
        floor_x = jnp.floor(pos_x)
        floor_y = jnp.floor(pos_y)
        tap_x = kaiser((taps - 2.0) - (pos_x - floor_x)).astype(jnp.bfloat16)
        tap_y = kaiser((taps - 2.0) - (pos_y - floor_y)).astype(jnp.bfloat16)
        tap_z = kaiser((taps - data[5:6]) - data[4:5])
        part_0 = tap_z * data[2:3]
        part_1 = tap_z * data[3:4]
        for z in range(PLANES):
            rowsc[z] = jnp.where(odd, part_1[z : z + 1], part_0[z : z + 1]).astype(jnp.bfloat16)
        cell_x = centred_cells(floor_x, taps_i, NX, row_base, rows // 2)
        cell_y = centred_cells(floor_y, taps_i, NY, 0, NY // 2)
        for r in range(0, rows, 8):
            wide_x[2 * r : 2 * r + 16] = widen(cell_x, tap_x, 2, 16, r - rows // 2)
        for r in range(0, NY, 128):
            wide_y[:, r : r + 128] = widen(cell_y, tap_y, 1, 128, r - NY // 2).T

        low, high = 0, 0
        for z in range(PLANES):
            low = low + (start[z + 6] <= first).astype(jnp.int32)
            high = high + (start[z] < first + CHUNK).astype(jnp.int32)

        def one_plane(z, carry):
            left = wide_x[...].reshape(rows // 8, 16, CHUNK) * rowsc[z][None]
            left = left.reshape(2 * rows, CHUNK)
            acc[z] += jnp.dot(left, wide_y[...], preferred_element_type=jnp.float32)
            return carry

        lax.fori_loop(low, high, one_plane, 0)
        return carry

    chunks = lax.div(start[LEVELS] + (CHUNK - 1), CHUNK)
    lax.fori_loop(0, chunks, one_chunk, 0)

    copies = []
    for z in range(PLANES):
        stage[z] = acc[z].reshape(rows, 2, NY)
        copy = pltpu.make_async_copy(stage.at[z], out.at[:, z], sems.at[z])
        copy.start()
        copies.append(copy)
    for copy in copies:
        copy.wait()


def solution(mesh):
    groups = mesh.shape["grp"]
    slabs = mesh.shape["slab"]
    rows = NX // groups

    def shards(sample_xy, sample_dz, sample_values, block_tile, block_count):
        blocks, _, length = sample_xy.shape[2:]
        own = (
            sample_xy.reshape(blocks, 2, length),
            sample_dz.reshape(blocks, length),
            sample_values.reshape(blocks, 2, length),
            block_tile.reshape(1, blocks),
            block_count.reshape(1, blocks),
        )
        copies = 5 * (3 * groups - 1)
        gathered = pl.pallas_call(
            lambda *refs: exchange(groups, slabs, *refs),
            out_shape=[jax.ShapeDtypeStruct((3, groups) + a.shape, a.dtype) for a in own],
            in_specs=[pl.BlockSpec(memory_space=pltpu.VMEM)] * 5,
            out_specs=[pl.BlockSpec(memory_space=pl.ANY)] * 5,
            scratch_shapes=[pltpu.SemaphoreType.DMA((count,)) for count in (copies, copies, 5)],
            compiler_params=pltpu.CompilerParams(collective_id=0, has_side_effects=True),
        )(*own)
        slots = 3 * groups * blocks * length
        return pl.pallas_call(
            lambda *refs: grid_kernel(groups, rows, *refs),
            out_shape=jax.ShapeDtypeStruct((rows, PLANES, 2, NY), jnp.float32),
            in_specs=[pl.BlockSpec(memory_space=pltpu.VMEM)] * 3
            + [pl.BlockSpec(memory_space=pltpu.SMEM)] * 2,
            out_specs=pl.BlockSpec(memory_space=pl.ANY),
            scratch_shapes=[
                pltpu.VMEM((8, slots + 2 * CHUNK), jnp.float32),
                pltpu.VMEM((PLANES, 2 * rows, NY), jnp.float32),
                pltpu.VMEM((2 * rows, CHUNK), jnp.bfloat16),
                pltpu.VMEM((CHUNK, NY), jnp.bfloat16),
                pltpu.VMEM((PLANES, 16, CHUNK), jnp.bfloat16),
                pltpu.VMEM((PLANES, rows, 2, NY), jnp.float32),
                pltpu.SMEM((LEVELS + 1,), jnp.int32),
                pltpu.SMEM((LEVELS + 1,), jnp.int32),
                pltpu.SemaphoreType.DMA((PLANES,)),
            ],
            compiler_params=pltpu.CompilerParams(vmem_limit_bytes=60 * 1024 * 1024),
        )(*gathered)

    return jax.shard_map(
        shards,
        mesh=mesh,
        in_specs=(
            P("grp", "slab", None, None, None),
            P("grp", "slab", None, None),
            P("grp", "slab", None, None, None),
            P("grp", "slab", None),
            P("grp", "slab", None),
        ),
        out_specs=P("grp", "slab", None, None),
        check_vma=False,
    )
```

```python
import math

import jax
import jax.numpy as jnp
from jax import lax
from jax.experimental import pallas as pl
from jax.experimental.pallas import tpu as pltpu
from jax.sharding import PartitionSpec as P

NX = 384
NY = 384
PLANES = 6
REACH = 3
LEVELS = PLANES + 5
CHUNK = 256
LANES = 128

BETA = math.pi * math.sqrt(19.45)
MESH = pl.DeviceIdType.MESH


def kaiser_coefs():
    half_sq = (0.5 * BETA) ** 2
    term = 1.0
    terms = []
    for order in range(1, 32):
        term = term * half_sq / (order * order)
        terms.append(term)
    top = sum(terms)
    return [value / top for value in terms]


COEFS = kaiser_coefs()


def kaiser(distance):
    scaled = distance * (1.0 / 3.0)
    inside = jnp.maximum(1.0 - scaled * scaled, 0.0)
    total = jnp.full_like(inside, COEFS[-1])
    for coef in COEFS[-2::-1]:
        total = total * inside + coef
    return total * inside


def split_parts(value):
    parts = []
    for _ in range(3):
        part = value.astype(jnp.bfloat16)
        parts.append(part)
        value = value - part.astype(jnp.float32)
    return parts


def exchange(groups, slabs, rows, xy, dz, val, tile, cnt, out, meta, packed, info, send_sem, recv_sem, self_sem):
    blocks, _, length = xy.shape
    grp = lax.axis_index("grp")
    slab = lax.axis_index("slab")
    partners = []
    for side in range(3):
        for hop in range(groups):
            if side != 1 or hop != 0:
                partners.append(
                    (side, lax.rem(grp + hop, groups), lax.rem(slab + slabs + 1 - side, slabs))
                )
    barrier = pltpu.get_barrier_semaphore()
    for _, g, j in partners:
        pl.semaphore_signal(barrier, inc=1, device_id=(g, j), device_id_type=MESH)

    slot = lax.broadcasted_iota(jnp.int32, (1, length), 1)
    upto = (
        lax.broadcasted_iota(jnp.int32, (length, length), 0)
        <= lax.broadcasted_iota(jnp.int32, (length, length), 1)
    ).astype(jnp.float32).astype(jnp.bfloat16)
    place = lax.broadcasted_iota(jnp.int32, (length, length), 0)
    place = place.astype(jnp.float32).astype(jnp.bfloat16)
    lane = lax.broadcasted_iota(jnp.int32, (1, LANES), 1)
    terms = []
    reach = [[] for _ in range(groups)]
    for b in range(blocks):
        data = jnp.concatenate([xy[b], val[b], dz[b : b + 1]], axis=0)
        terms.append(jnp.concatenate(split_parts(data), axis=0))
        first = jnp.floor(xy[b, 0:1]).astype(jnp.int32) - 2
        used = slot < cnt[0, b]
        for g in range(groups):
            ahead = first + (5 - g * rows)
            ahead = jnp.where(ahead < 0, ahead + NX, ahead)
            ahead = jnp.where(ahead >= NX, ahead - NX, ahead)
            reach[g].append((used & (ahead < rows + 5)).astype(jnp.float32))
    for g in range(groups):
        mask = jnp.concatenate(reach[g], axis=0)
        rank = jnp.dot(mask.astype(jnp.bfloat16), upto, preferred_element_type=jnp.float32)
        kept = rank[:, length - 1 : length].astype(jnp.int32)
        goal = jnp.where(mask > 0.0, rank - 1.0, -1.0).astype(jnp.bfloat16)
        for b in range(blocks):
            move = jnp.where(
                place == goal[b : b + 1], jnp.ones_like(place), jnp.zeros_like(place)
            )
            moved = lax.dot_general(
                terms[b], move, (((1,), (1,)), ((), ())), preferred_element_type=jnp.float32
            )
            packed[g, b, 0:5] = (moved[0:5] + moved[5:10]) + moved[10:15]
            packed[g, b, 5:8] = jnp.zeros((3, length), jnp.float32)
            info[g, b : b + 1] = jnp.where(lane == 0, kept[b : b + 1], tile[0, b])

    pl.semaphore_wait(barrier, len(partners))
    own = [
        pltpu.make_async_copy(packed.at[grp], out.at[1, grp], self_sem.at[0]),
        pltpu.make_async_copy(info.at[grp], meta.at[1, grp], self_sem.at[1]),
    ]
    copies = []
    for side, g, j in partners:
        for src, dst in ((packed, out), (info, meta)):
            copies.append(
                pltpu.make_async_remote_copy(
                    src_ref=src.at[g],
                    dst_ref=dst.at[side, grp],
                    send_sem=send_sem.at[len(copies)],
                    recv_sem=recv_sem.at[len(copies)],
                    device_id=(g, j),
                    device_id_type=MESH,
                )
            )
            copies[-1].start()
    for copy in own:
        copy.start()
    for copy in own + copies:
        copy.wait()


def widen(cells, weights, repeat, count, first):
    ids = lax.broadcasted_iota(jnp.int32, (count, CHUNK), 0)
    ids = (lax.div(ids, repeat) + first).astype(jnp.float32).astype(jnp.bfloat16)
    wide = jnp.zeros((count, CHUNK), jnp.bfloat16)
    for k in range(6):
        wide = jnp.where(ids == cells[k : k + 1], weights[k : k + 1], wide)
    return wide


def centred_cells(floor, taps_i, period, base, half):
    cell = floor.astype(jnp.int32) - 2 + taps_i
    cell = jnp.where(cell < 0, cell + period, cell)
    cell = jnp.where(cell >= period, cell - period, cell) - (base + half)
    cell = jnp.where((cell >= -half) & (cell < half), cell, 256)
    return cell.astype(jnp.float32).astype(jnp.bfloat16)


def grid_kernel(
    groups, rows, packed, meta, out, comp, acc, wide_x, wide_y, rowsc, stage, start, cursor, sems
):
    blocks = packed.shape[2]
    row_base = lax.axis_index("grp") * rows

    for level in range(LEVELS + 2):
        start[level] = 0
    comp[...] = jnp.zeros_like(comp)

    def each_block(visit):
        for side in range(3):

            def one_group(g, carry, side=side):
                for b in range(blocks):
                    level = meta[side, g, b, 1] + (PLANES * (side - 1) + REACH)
                    visit(side, g, b, level, meta[side, g, b, 0])
                return carry

            lax.fori_loop(0, groups, one_group, 0)

    def count(side, g, b, level, used):
        if side == 1:
            start[level + 1] = start[level + 1] + used
        else:
            inside = (level >= 0) & (level < LEVELS)
            at = jnp.where(inside, level + 1, LEVELS + 1)
            start[at] = start[at] + used

    each_block(count)
    cursor[0] = 0
    for level in range(1, LEVELS + 1):
        start[level] = start[level] + start[level - 1]
        cursor[level] = start[level]

    lane = lax.broadcasted_iota(jnp.int32, (8, LANES), 1)
    sublane = lax.broadcasted_iota(jnp.int32, (8, 2 * LANES), 0)

    def place(side, g, b, level, used):
        @pl.when((level >= 0) & (level < LEVELS) & (used > 0))
        def _():
            to = cursor[level]
            cursor[level] = to + used
            shift = lax.rem(to, LANES)
            base = pl.multiple_of(to - shift, LANES)
            data = packed[side, g, b]
            plane = (level - REACH).astype(jnp.float32)
            data = jnp.where(sublane == 5, plane, data)
            pieces = [
                pltpu.roll(data[:, p * LANES : (p + 1) * LANES], shift, axis=1)
                for p in range(data.shape[1] // LANES)
            ]
            for p in range(len(pieces) + 1):
                before = pieces[max(p - 1, 0)]
                after = pieces[min(p, len(pieces) - 1)]
                merged = jnp.where(lane < shift, before, after)
                slot = lane + (p * LANES - shift)
                at_lanes = pl.ds(base + p * LANES, LANES)
                comp[:, at_lanes] = jnp.where(
                    (slot >= 0) & (slot < used), merged, comp[:, at_lanes]
                )

    each_block(place)
    acc[...] = jnp.zeros_like(acc)

    taps_i = lax.broadcasted_iota(jnp.int32, (8, CHUNK), 0)
    taps = taps_i.astype(jnp.float32)
    odd = (lax.broadcasted_iota(jnp.int32, (16, CHUNK), 0) & 1) == 1

    def one_chunk(i, carry):
        first = i * CHUNK
        data = comp[:, pl.ds(pl.multiple_of(first, CHUNK), CHUNK)]
        pos_x, pos_y = data[0:1], data[1:2]
        floor_x = jnp.floor(pos_x)
        floor_y = jnp.floor(pos_y)
        tap_x = kaiser((taps - 2.0) - (pos_x - floor_x)).astype(jnp.bfloat16)
        tap_y = kaiser((taps - 2.0) - (pos_y - floor_y)).astype(jnp.bfloat16)
        tap_z = kaiser((taps - data[5:6]) - data[4:5])
        part_0 = tap_z * data[2:3]
        part_1 = tap_z * data[3:4]
        for z in range(PLANES):
            rowsc[z] = jnp.where(odd, part_1[z : z + 1], part_0[z : z + 1]).astype(jnp.bfloat16)
        cell_x = centred_cells(floor_x, taps_i, NX, row_base, rows // 2)
        cell_y = centred_cells(floor_y, taps_i, NY, 0, NY // 2)
        for r in range(0, rows, 8):
            wide_x[2 * r : 2 * r + 16] = widen(cell_x, tap_x, 2, 16, r - rows // 2)
        for r in range(0, NY, 128):
            wide_y[:, r : r + 128] = widen(cell_y, tap_y, 1, 128, r - NY // 2).T

        low, high = 0, 0
        for z in range(PLANES):
            low = low + (start[z + 6] <= first).astype(jnp.int32)
            high = high + (start[z] < first + CHUNK).astype(jnp.int32)

        def one_plane(z, carry):
            left = wide_x[...].reshape(rows // 8, 16, CHUNK) * rowsc[z][None]
            left = left.reshape(2 * rows, CHUNK)
            acc[z] += jnp.dot(left, wide_y[...], preferred_element_type=jnp.float32)
            return carry

        lax.fori_loop(low, high, one_plane, 0)
        return carry

    chunks = lax.div(start[LEVELS] + (CHUNK - 1), CHUNK)
    lax.fori_loop(0, chunks, one_chunk, 0)

    copies = []
    for z in range(PLANES):
        stage[z] = acc[z].reshape(rows, 2, NY)
        copy = pltpu.make_async_copy(stage.at[z], out.at[:, z], sems.at[z])
        copy.start()
        copies.append(copy)
    for copy in copies:
        copy.wait()


def solution(mesh):
    groups = mesh.shape["grp"]
    slabs = mesh.shape["slab"]
    rows = NX // groups

    def shards(sample_xy, sample_dz, sample_values, block_tile, block_count):
        blocks, _, length = sample_xy.shape[2:]
        own = (
            sample_xy.reshape(blocks, 2, length),
            sample_dz.reshape(blocks, length),
            sample_values.reshape(blocks, 2, length),
            block_tile.reshape(1, blocks),
            block_count.reshape(1, blocks),
        )
        copies = 2 * (3 * groups - 1)
        gathered = pl.pallas_call(
            lambda *refs: exchange(groups, slabs, rows, *refs),
            out_shape=[
                jax.ShapeDtypeStruct((3, groups, blocks, 8, length), jnp.float32),
                jax.ShapeDtypeStruct((3, groups, blocks, LANES), jnp.int32),
            ],
            in_specs=[pl.BlockSpec(memory_space=pltpu.VMEM)] * 3
            + [pl.BlockSpec(memory_space=pltpu.SMEM)] * 2,
            out_specs=[pl.BlockSpec(memory_space=pl.ANY)] * 2,
            scratch_shapes=[
                pltpu.VMEM((groups, blocks, 8, length), jnp.float32),
                pltpu.VMEM((groups, blocks, LANES), jnp.int32),
            ]
            + [pltpu.SemaphoreType.DMA((count,)) for count in (copies, copies, 2)],
            compiler_params=pltpu.CompilerParams(collective_id=0, has_side_effects=True),
        )(*own)
        slots = 3 * groups * blocks * length
        return pl.pallas_call(
            lambda *refs: grid_kernel(groups, rows, *refs),
            out_shape=jax.ShapeDtypeStruct((rows, PLANES, 2, NY), jnp.float32),
            in_specs=[
                pl.BlockSpec(memory_space=pltpu.VMEM),
                pl.BlockSpec(memory_space=pltpu.SMEM),
            ],
            out_specs=pl.BlockSpec(memory_space=pl.ANY),
            scratch_shapes=[
                pltpu.VMEM((8, slots + 2 * CHUNK), jnp.float32),
                pltpu.VMEM((PLANES, 2 * rows, NY), jnp.float32),
                pltpu.VMEM((2 * rows, CHUNK), jnp.bfloat16),
                pltpu.VMEM((CHUNK, NY), jnp.bfloat16),
                pltpu.VMEM((PLANES, 16, CHUNK), jnp.bfloat16),
                pltpu.VMEM((PLANES, rows, 2, NY), jnp.float32),
                pltpu.SMEM((LEVELS + 2,), jnp.int32),
                pltpu.SMEM((LEVELS + 1,), jnp.int32),
                pltpu.SemaphoreType.DMA((PLANES,)),
            ],
            compiler_params=pltpu.CompilerParams(vmem_limit_bytes=60 * 1024 * 1024),
        )(*gathered)

    return jax.shard_map(
        shards,
        mesh=mesh,
        in_specs=(
            P("grp", "slab", None, None, None),
            P("grp", "slab", None, None),
            P("grp", "slab", None, None, None),
            P("grp", "slab", None),
            P("grp", "slab", None),
        ),
        out_specs=P("grp", "slab", None, None),
        check_vma=False,
    )
```

```python
import math

import jax
import jax.numpy as jnp
from jax import lax
from jax.experimental import pallas as pl
from jax.experimental.pallas import tpu as pltpu
from jax.sharding import PartitionSpec as P

NX = 384
NY = 384
PLANES = 6
REACH = 3
LEVELS = PLANES + 5
CHUNK = 256
LANES = 128

BETA = math.pi * math.sqrt(19.45)
MESH = pl.DeviceIdType.MESH


def kaiser_coefs():
    half_sq = (0.5 * BETA) ** 2
    term = 1.0
    terms = []
    for order in range(1, 32):
        term = term * half_sq / (order * order)
        terms.append(term)
    top = sum(terms)
    return [value / top for value in terms]


COEFS = kaiser_coefs()


def kaiser(distance):
    scaled = distance * (1.0 / 3.0)
    inside = jnp.maximum(1.0 - scaled * scaled, 0.0)
    total = jnp.full_like(inside, COEFS[-1])
    for coef in COEFS[-2::-1]:
        total = total * inside + coef
    return total * inside


def split_parts(value):
    parts = []
    for _ in range(3):
        part = value.astype(jnp.bfloat16)
        parts.append(part)
        value = value - part.astype(jnp.float32)
    return parts


def exchange(groups, slabs, rows, xy, dz, val, tile, cnt, out, meta, packed, info, send_sem, recv_sem, self_sem):
    blocks, _, length = xy.shape
    grp = lax.axis_index("grp")
    slab = lax.axis_index("slab")
    partners = []
    for side in range(3):
        for hop in range(groups):
            if side != 1 or hop != 0:
                partners.append(
                    (side, lax.rem(grp + hop, groups), lax.rem(slab + slabs + 1 - side, slabs))
                )
    barrier = pltpu.get_barrier_semaphore()
    for _, g, j in partners:
        pl.semaphore_signal(barrier, inc=1, device_id=(g, j), device_id_type=MESH)

    slot = lax.broadcasted_iota(jnp.int32, (1, length), 1)
    upto = (
        lax.broadcasted_iota(jnp.int32, (length, length), 0)
        <= lax.broadcasted_iota(jnp.int32, (length, length), 1)
    ).astype(jnp.float32).astype(jnp.bfloat16)
    place = lax.broadcasted_iota(jnp.int32, (length, length), 0)
    place = place.astype(jnp.float32).astype(jnp.bfloat16)
    lane = lax.broadcasted_iota(jnp.int32, (1, LANES), 1)
    terms = []
    reach = [[] for _ in range(groups)]
    for b in range(blocks):
        data = jnp.concatenate([xy[b], val[b], dz[b : b + 1]], axis=0)
        terms.append(jnp.concatenate(split_parts(data), axis=0))
        first = jnp.floor(xy[b, 0:1]).astype(jnp.int32) - 2
        used = slot < cnt[0, b]
        for g in range(groups):
            ahead = first + (5 - g * rows)
            ahead = jnp.where(ahead < 0, ahead + NX, ahead)
            ahead = jnp.where(ahead >= NX, ahead - NX, ahead)
            reach[g].append((used & (ahead < rows + 5)).astype(jnp.float32))
    for g in range(groups):
        mask = jnp.concatenate(reach[g], axis=0)
        rank = jnp.dot(mask.astype(jnp.bfloat16), upto, preferred_element_type=jnp.float32)
        kept = rank[:, length - 1 : length].astype(jnp.int32)
        goal = jnp.where(mask > 0.0, rank - 1.0, -1.0).astype(jnp.bfloat16)
        for b in range(blocks):
            move = jnp.where(
                place == goal[b : b + 1], jnp.ones_like(place), jnp.zeros_like(place)
            )
            moved = lax.dot_general(
                terms[b], move, (((1,), (1,)), ((), ())), preferred_element_type=jnp.float32
            )
            packed[g, b, 0:5] = (moved[0:5] + moved[5:10]) + moved[10:15]
            packed[g, b, 5:8] = jnp.zeros((3, length), jnp.float32)
            info[g, b : b + 1] = jnp.where(lane == 0, kept[b : b + 1], tile[0, b])

    pl.semaphore_wait(barrier, len(partners))
    own = [
        pltpu.make_async_copy(packed.at[grp], out.at[1, grp], self_sem.at[0]),
        pltpu.make_async_copy(info.at[grp], meta.at[1, grp], self_sem.at[1]),
    ]
    copies = []
    for side, g, j in partners:
        for src, dst in ((packed, out), (info, meta)):
            copies.append(
                pltpu.make_async_remote_copy(
                    src_ref=src.at[g],
                    dst_ref=dst.at[side, grp],
                    send_sem=send_sem.at[len(copies)],
                    recv_sem=recv_sem.at[len(copies)],
                    device_id=(g, j),
                    device_id_type=MESH,
                )
            )
            copies[-1].start()
    for copy in own:
        copy.start()
    for copy in own + copies:
        copy.wait()


def widen(cells, weights, repeat, count, first):
    ids = lax.broadcasted_iota(jnp.int32, (count, CHUNK), 0)
    ids = (lax.div(ids, repeat) + first).astype(jnp.float32).astype(jnp.bfloat16)
    wide = jnp.zeros((count, CHUNK), jnp.bfloat16)
    for k in range(6):
        wide = jnp.where(ids == cells[k : k + 1], weights[k : k + 1], wide)
    return wide


def centred_cells(floor, taps_i, period, base, half):
    cell = floor.astype(jnp.int32) - 2 + taps_i
    cell = jnp.where(cell < 0, cell + period, cell)
    cell = jnp.where(cell >= period, cell - period, cell) - (base + half)
    cell = jnp.where((cell >= -half) & (cell < half), cell, 256)
    return cell.astype(jnp.float32).astype(jnp.bfloat16)


def grid_kernel(
    groups, rows, packed_hbm, meta, out, packed, in_sem, comp, acc, wide_x, wide_y, rowsc, stage, start, cursor, sems
):
    blocks = packed.shape[2]
    fetch = pltpu.make_async_copy(packed_hbm, packed, in_sem)
    fetch.start()
    row_base = lax.axis_index("grp") * rows

    for level in range(LEVELS + 2):
        start[level] = 0
    comp[...] = jnp.zeros_like(comp)

    def each_block(visit):
        for side in range(3):

            def one_group(g, carry, side=side):
                for b in range(blocks):
                    level = meta[side, g, b, 1] + (PLANES * (side - 1) + REACH)
                    visit(side, g, b, level, meta[side, g, b, 0])
                return carry

            lax.fori_loop(0, groups, one_group, 0)

    def count(side, g, b, level, used):
        if side == 1:
            start[level + 1] = start[level + 1] + used
        else:
            inside = (level >= 0) & (level < LEVELS)
            at = jnp.where(inside, level + 1, LEVELS + 1)
            start[at] = start[at] + used

    each_block(count)
    cursor[0] = 0
    for level in range(1, LEVELS + 1):
        start[level] = start[level] + start[level - 1]
        cursor[level] = start[level]

    lane = lax.broadcasted_iota(jnp.int32, (8, LANES), 1)
    sublane = lax.broadcasted_iota(jnp.int32, (8, 2 * LANES), 0)

    def place(side, g, b, level, used):
        @pl.when((level >= 0) & (level < LEVELS) & (used > 0))
        def _():
            to = cursor[level]
            cursor[level] = to + used
            shift = lax.rem(to, LANES)
            base = pl.multiple_of(to - shift, LANES)
            data = packed[side, g, b]
            plane = (level - REACH).astype(jnp.float32)
            data = jnp.where(sublane == 5, plane, data)
            pieces = [
                pltpu.roll(data[:, p * LANES : (p + 1) * LANES], shift, axis=1)
                for p in range(data.shape[1] // LANES)
            ]
            for p in range(len(pieces) + 1):
                before = pieces[max(p - 1, 0)]
                after = pieces[min(p, len(pieces) - 1)]
                merged = jnp.where(lane < shift, before, after)
                slot = lane + (p * LANES - shift)
                at_lanes = pl.ds(base + p * LANES, LANES)
                comp[:, at_lanes] = jnp.where(
                    (slot >= 0) & (slot < used), merged, comp[:, at_lanes]
                )

    acc[...] = jnp.zeros_like(acc)
    fetch.wait()
    each_block(place)

    taps_i = lax.broadcasted_iota(jnp.int32, (8, CHUNK), 0)
    taps = taps_i.astype(jnp.float32)
    odd = (lax.broadcasted_iota(jnp.int32, (16, CHUNK), 0) & 1) == 1

    def one_chunk(i, carry):
        first = i * CHUNK
        data = comp[:, pl.ds(pl.multiple_of(first, CHUNK), CHUNK)]
        pos_x, pos_y = data[0:1], data[1:2]
        floor_x = jnp.floor(pos_x)
        floor_y = jnp.floor(pos_y)
        tap_x = kaiser((taps - 2.0) - (pos_x - floor_x)).astype(jnp.bfloat16)
        tap_y = kaiser((taps - 2.0) - (pos_y - floor_y)).astype(jnp.bfloat16)
        tap_z = kaiser((taps - data[5:6]) - data[4:5])
        part_0 = tap_z * data[2:3]
        part_1 = tap_z * data[3:4]
        for z in range(PLANES + 1):
            rowsc[z] = jnp.where(odd, part_1[z : z + 1], part_0[z : z + 1]).astype(jnp.bfloat16)
        cell_x = centred_cells(floor_x, taps_i, NX, row_base, rows // 2)
        cell_y = centred_cells(floor_y, taps_i, NY, 0, NY // 2)
        for r in range(0, rows, 8):
            wide_x[2 * r : 2 * r + 16] = widen(cell_x, tap_x, 2, 16, r - rows // 2)
        for r in range(0, NY, 128):
            wide_y[:, r : r + 128] = widen(cell_y, tap_y, 1, 128, r - NY // 2).T

        low, high, done = 0, 0, 0
        for z in range(PLANES):
            low = low + (start[z + 6] <= first).astype(jnp.int32)
            high = high + (start[z] < first + CHUNK).astype(jnp.int32)
            done = done + (start[z + 6] <= first + CHUNK).astype(jnp.int32)

        def two_planes(t, carry):
            z = low + 2 * t
            left = wide_x[...].reshape(1, rows // 8, 16, CHUNK) * rowsc[pl.ds(z, 2)][:, None]
            at_rows = pl.ds(pl.multiple_of(z * 2 * rows, 2 * rows), 4 * rows)
            acc[at_rows] += jnp.dot(
                left.reshape(4 * rows, CHUNK), wide_y[...], preferred_element_type=jnp.float32
            )
            return carry

        lax.fori_loop(0, lax.div(high - low + 1, 2), two_planes, 0)

        def put(z, carry):
            at_rows = pl.ds(pl.multiple_of(z * 2 * rows, 2 * rows), 2 * rows)
            stage[z] = acc[at_rows].reshape(rows, 2, NY)
            pltpu.make_async_copy(stage.at[z], out.at[:, z], sems.at[z]).start()
            return carry

        lax.fori_loop(jnp.where(i == 0, 0, low), done, put, 0)
        return carry

    chunks = lax.div(start[LEVELS] + (CHUNK - 1), CHUNK)
    lax.fori_loop(0, jnp.maximum(chunks, 1), one_chunk, 0)

    for z in range(PLANES):
        pltpu.make_async_copy(stage.at[z], out.at[:, z], sems.at[z]).wait()


def solution(mesh):
    groups = mesh.shape["grp"]
    slabs = mesh.shape["slab"]
    rows = NX // groups

    def shards(sample_xy, sample_dz, sample_values, block_tile, block_count):
        blocks, _, length = sample_xy.shape[2:]
        own = (
            sample_xy.reshape(blocks, 2, length),
            sample_dz.reshape(blocks, length),
            sample_values.reshape(blocks, 2, length),
            block_tile.reshape(1, blocks),
            block_count.reshape(1, blocks),
        )
        copies = 2 * (3 * groups - 1)
        gathered = pl.pallas_call(
            lambda *refs: exchange(groups, slabs, rows, *refs),
            out_shape=[
                jax.ShapeDtypeStruct((3, groups, blocks, 8, length), jnp.float32),
                jax.ShapeDtypeStruct((3, groups, blocks, LANES), jnp.int32),
            ],
            in_specs=[pl.BlockSpec(memory_space=pltpu.VMEM)] * 3
            + [pl.BlockSpec(memory_space=pltpu.SMEM)] * 2,
            out_specs=[pl.BlockSpec(memory_space=pl.ANY)] * 2,
            scratch_shapes=[
                pltpu.VMEM((groups, blocks, 8, length), jnp.float32),
                pltpu.VMEM((groups, blocks, LANES), jnp.int32),
            ]
            + [pltpu.SemaphoreType.DMA((count,)) for count in (copies, copies, 2)],
            compiler_params=pltpu.CompilerParams(collective_id=0, has_side_effects=True),
        )(*own)
        slots = 3 * groups * blocks * length
        return pl.pallas_call(
            lambda *refs: grid_kernel(groups, rows, *refs),
            out_shape=jax.ShapeDtypeStruct((rows, PLANES, 2, NY), jnp.float32),
            in_specs=[
                pl.BlockSpec(memory_space=pl.ANY),
                pl.BlockSpec(memory_space=pltpu.SMEM),
            ],
            out_specs=pl.BlockSpec(memory_space=pl.ANY),
            scratch_shapes=[
                pltpu.VMEM((3, groups, blocks, 8, length), jnp.float32),
                pltpu.SemaphoreType.DMA,
                pltpu.VMEM((8, slots + 2 * CHUNK), jnp.float32),
                pltpu.VMEM(((PLANES + 1) * 2 * rows, NY), jnp.float32),
                pltpu.VMEM((2 * rows, CHUNK), jnp.bfloat16),
                pltpu.VMEM((CHUNK, NY), jnp.bfloat16),
                pltpu.VMEM((PLANES + 1, 16, CHUNK), jnp.bfloat16),
                pltpu.VMEM((PLANES, rows, 2, NY), jnp.float32),
                pltpu.SMEM((LEVELS + 2,), jnp.int32),
                pltpu.SMEM((LEVELS + 1,), jnp.int32),
                pltpu.SemaphoreType.DMA((PLANES,)),
            ],
            compiler_params=pltpu.CompilerParams(vmem_limit_bytes=60 * 1024 * 1024),
        )(*gathered)

    return jax.shard_map(
        shards,
        mesh=mesh,
        in_specs=(
            P("grp", "slab", None, None, None),
            P("grp", "slab", None, None),
            P("grp", "slab", None, None, None),
            P("grp", "slab", None),
            P("grp", "slab", None),
        ),
        out_specs=P("grp", "slab", None, None),
        check_vma=False,
    )
```

```python
import math

import jax
import jax.numpy as jnp
from jax import lax
from jax.experimental import pallas as pl
from jax.experimental.pallas import tpu as pltpu
from jax.sharding import PartitionSpec as P

NX = 384
NY = 384
PLANES = 6
REACH = 3
LEVELS = PLANES + 5
CHUNK = 256
LANES = 128

BETA = math.pi * math.sqrt(19.45)
MESH = pl.DeviceIdType.MESH


def kaiser_coefs():
    half_sq = (0.5 * BETA) ** 2
    term = 1.0
    terms = []
    for order in range(1, 32):
        term = term * half_sq / (order * order)
        terms.append(term)
    top = sum(terms)
    return [value / top for value in terms]


COEFS = kaiser_coefs()


def kaiser(distance):
    scaled = distance * (1.0 / 3.0)
    inside = jnp.maximum(1.0 - scaled * scaled, 0.0)
    total = jnp.full_like(inside, COEFS[-1])
    for coef in COEFS[-2::-1]:
        total = total * inside + coef
    return total * inside


def split_parts(value):
    parts = []
    for _ in range(3):
        part = value.astype(jnp.bfloat16)
        parts.append(part)
        value = value - part.astype(jnp.float32)
    return parts


def exchange(groups, slabs, rows, xy, dz, val, tile, cnt, out, meta, packed, info, send_sem, recv_sem, self_sem):
    blocks, _, length = xy.shape
    grp = lax.axis_index("grp")
    slab = lax.axis_index("slab")
    partners = []
    for side in range(3):
        for hop in range(groups):
            if side != 1 or hop != 0:
                partners.append(
                    (side, lax.rem(grp + hop, groups), lax.rem(slab + slabs + 1 - side, slabs))
                )
    barrier = pltpu.get_barrier_semaphore()
    for _, g, j in partners:
        pl.semaphore_signal(barrier, inc=1, device_id=(g, j), device_id_type=MESH)

    slot = lax.broadcasted_iota(jnp.int32, (1, length), 1)
    upto = (
        lax.broadcasted_iota(jnp.int32, (length, length), 0)
        <= lax.broadcasted_iota(jnp.int32, (length, length), 1)
    ).astype(jnp.float32).astype(jnp.bfloat16)
    place = lax.broadcasted_iota(jnp.int32, (length, length), 0)
    place = place.astype(jnp.float32).astype(jnp.bfloat16)
    lane = lax.broadcasted_iota(jnp.int32, (1, LANES), 1)
    terms = []
    reach = [[] for _ in range(groups)]
    for b in range(blocks):
        data = jnp.concatenate([xy[b], val[b], dz[b : b + 1]], axis=0)
        terms.append(jnp.concatenate(split_parts(data), axis=0))
        first = jnp.floor(xy[b, 0:1]).astype(jnp.int32) - 2
        used = slot < cnt[0, b]
        for g in range(groups):
            ahead = first + (5 - g * rows)
            ahead = jnp.where(ahead < 0, ahead + NX, ahead)
            ahead = jnp.where(ahead >= NX, ahead - NX, ahead)
            reach[g].append((used & (ahead < rows + 5)).astype(jnp.float32))
    for g in range(groups):
        mask = jnp.concatenate(reach[g], axis=0)
        rank = jnp.dot(mask.astype(jnp.bfloat16), upto, preferred_element_type=jnp.float32)
        kept = rank[:, length - 1 : length].astype(jnp.int32)
        goal = jnp.where(mask > 0.0, rank - 1.0, -1.0).astype(jnp.bfloat16)
        for b in range(blocks):
            move = jnp.where(
                place == goal[b : b + 1], jnp.ones_like(place), jnp.zeros_like(place)
            )
            moved = lax.dot_general(
                terms[b], move, (((1,), (1,)), ((), ())), preferred_element_type=jnp.float32
            )
            packed[g, 5 * b : 5 * b + 5] = (moved[0:5] + moved[5:10]) + moved[10:15]
            info[g, b : b + 1] = jnp.where(lane == 0, kept[b : b + 1], tile[0, b])

    pl.semaphore_wait(barrier, len(partners))
    own = [
        pltpu.make_async_copy(packed.at[grp], out.at[1, grp], self_sem.at[0]),
        pltpu.make_async_copy(info.at[grp], meta.at[1, grp], self_sem.at[1]),
    ]
    copies = []
    for side, g, j in partners:
        for src, dst in ((packed, out), (info, meta)):
            copies.append(
                pltpu.make_async_remote_copy(
                    src_ref=src.at[g],
                    dst_ref=dst.at[side, grp],
                    send_sem=send_sem.at[len(copies)],
                    recv_sem=recv_sem.at[len(copies)],
                    device_id=(g, j),
                    device_id_type=MESH,
                )
            )
            copies[-1].start()
    for copy in own:
        copy.start()
    for copy in own + copies:
        copy.wait()


def widen(cells, weights, repeat, count, first):
    ids = lax.div(lax.broadcasted_iota(jnp.int32, (16, CHUNK), 0), repeat)
    ids = ids.astype(jnp.float32).astype(jnp.bfloat16)
    ids = [ids + jnp.bfloat16(first + at // repeat) for at in range(0, count, 16)]
    ids = jnp.concatenate(ids, axis=0)
    wide = jnp.zeros((count, CHUNK), jnp.bfloat16)
    for k in range(6):
        wide = jnp.where(ids == cells[k : k + 1], weights[k : k + 1], wide)
    return wide


def centred_cells(floor, taps_i, period, base, half):
    cell = floor.astype(jnp.int32) - 2 + taps_i
    cell = jnp.where(cell < 0, cell + period, cell)
    cell = jnp.where(cell >= period, cell - period, cell) - (base + half)
    cell = jnp.where((cell >= -half) & (cell < half), cell, 256)
    return cell.astype(jnp.float32).astype(jnp.bfloat16)


def grid_kernel(
    groups, rows, packed_hbm, meta, out, packed, in_sem, comp, acc, wide_x, wide_y, rowsc, stage, start, cursor, sems
):
    blocks = packed.shape[2] // 5
    fetch = pltpu.make_async_copy(packed_hbm, packed, in_sem)
    fetch.start()
    row_base = lax.axis_index("grp") * rows

    for level in range(LEVELS + 2):
        start[level] = 0
    comp[...] = jnp.zeros_like(comp)

    def each_block(visit):
        for side in range(3):

            def one_group(g, carry, side=side):
                for b in range(blocks):
                    level = meta[side, g, b, 1] + (PLANES * (side - 1) + REACH)
                    visit(side, g, b, level, meta[side, g, b, 0])
                return carry

            lax.fori_loop(0, groups, one_group, 0)

    def count(side, g, b, level, used):
        if side == 1:
            start[level + 1] = start[level + 1] + used
        else:
            inside = (level >= 0) & (level < LEVELS)
            at = jnp.where(inside, level + 1, LEVELS + 1)
            start[at] = start[at] + used

    each_block(count)
    cursor[0] = 0
    for level in range(1, LEVELS + 1):
        start[level] = start[level] + start[level - 1]
        cursor[level] = start[level]

    lane = lax.broadcasted_iota(jnp.int32, (8, LANES), 1)
    sublane = lax.broadcasted_iota(jnp.int32, (8, 2 * LANES), 0)

    def place(side, g, b, level, used):
        @pl.when((level >= 0) & (level < LEVELS) & (used > 0))
        def _():
            to = cursor[level]
            cursor[level] = to + used
            shift = lax.rem(to, LANES)
            base = pl.multiple_of(to - shift, LANES)
            data = packed[side, g, 5 * b : 5 * b + 5]
            data = jnp.concatenate([data, data[:3]], axis=0)
            plane = (level - REACH).astype(jnp.float32)
            data = jnp.where(sublane == 5, plane, data)
            pieces = [
                pltpu.roll(data[:, p * LANES : (p + 1) * LANES], shift, axis=1)
                for p in range(data.shape[1] // LANES)
            ]
            for p in range(len(pieces) + 1):
                before = pieces[max(p - 1, 0)]
                after = pieces[min(p, len(pieces) - 1)]
                merged = jnp.where(lane < shift, before, after)
                slot = lane + (p * LANES - shift)
                at_lanes = pl.ds(base + p * LANES, LANES)
                comp[:, at_lanes] = jnp.where(
                    (slot >= 0) & (slot < used), merged, comp[:, at_lanes]
                )

    acc[...] = jnp.zeros_like(acc)
    fetch.wait()
    each_block(place)

    taps_i = lax.broadcasted_iota(jnp.int32, (8, CHUNK), 0)
    taps = taps_i.astype(jnp.float32)
    odd = (lax.broadcasted_iota(jnp.int32, (16, CHUNK), 0) & 1) == 1

    def one_chunk(i, carry):
        first = i * CHUNK
        data = comp[:, pl.ds(pl.multiple_of(first, CHUNK), CHUNK)]
        pos_x, pos_y = data[0:1], data[1:2]
        floor_x = jnp.floor(pos_x)
        floor_y = jnp.floor(pos_y)
        tap_x = kaiser((taps - 2.0) - (pos_x - floor_x)).astype(jnp.bfloat16)
        tap_y = kaiser((taps - 2.0) - (pos_y - floor_y)).astype(jnp.bfloat16)
        tap_z = kaiser((taps - data[5:6]) - data[4:5])
        part_0 = tap_z * data[2:3]
        part_1 = tap_z * data[3:4]
        for z in range(PLANES + 1):
            rowsc[z] = jnp.where(odd, part_1[z : z + 1], part_0[z : z + 1]).astype(jnp.bfloat16)
        cell_x = centred_cells(floor_x, taps_i, NX, row_base, rows // 2)
        cell_y = centred_cells(floor_y, taps_i, NY, 0, NY // 2)
        for r in range(0, rows, 8):
            wide_x[2 * r : 2 * r + 16] = widen(cell_x, tap_x, 2, 16, r - rows // 2)
        for r in range(0, NY, 128):
            wide_y[:, r : r + 128] = widen(cell_y, tap_y, 1, 128, r - NY // 2).T

        low, high, done = 0, 0, 0
        for z in range(PLANES):
            low = low + (start[z + 6] <= first).astype(jnp.int32)
            high = high + (start[z] < first + CHUNK).astype(jnp.int32)
            done = done + (start[z + 6] <= first + CHUNK).astype(jnp.int32)

        def two_planes(t, carry):
            z = low + 2 * t
            left = wide_x[...].reshape(1, rows // 8, 16, CHUNK) * rowsc[pl.ds(z, 2)][:, None]
            at_rows = pl.ds(pl.multiple_of(z * 2 * rows, 2 * rows), 4 * rows)
            acc[at_rows] += jnp.dot(
                left.reshape(4 * rows, CHUNK), wide_y[...], preferred_element_type=jnp.float32
            )
            return carry

        lax.fori_loop(0, lax.div(high - low + 1, 2), two_planes, 0)

        def put(z, carry):
            at_rows = pl.ds(pl.multiple_of(z * 2 * rows, 2 * rows), 2 * rows)
            stage[z] = acc[at_rows].reshape(rows, 2, NY)
            pltpu.make_async_copy(stage.at[z], out.at[:, z], sems.at[z]).start()
            return carry

        lax.fori_loop(jnp.where(i == 0, 0, low), done, put, 0)
        return carry

    chunks = lax.div(start[LEVELS] + (CHUNK - 1), CHUNK)
    lax.fori_loop(0, jnp.maximum(chunks, 1), one_chunk, 0)

    for z in range(PLANES):
        pltpu.make_async_copy(stage.at[z], out.at[:, z], sems.at[z]).wait()


def solution(mesh):
    groups = mesh.shape["grp"]
    slabs = mesh.shape["slab"]
    rows = NX // groups

    def shards(sample_xy, sample_dz, sample_values, block_tile, block_count):
        blocks, _, length = sample_xy.shape[2:]
        own = (
            sample_xy.reshape(blocks, 2, length),
            sample_dz.reshape(blocks, length),
            sample_values.reshape(blocks, 2, length),
            block_tile.reshape(1, blocks),
            block_count.reshape(1, blocks),
        )
        copies = 2 * (3 * groups - 1)
        gathered = pl.pallas_call(
            lambda *refs: exchange(groups, slabs, rows, *refs),
            out_shape=[
                jax.ShapeDtypeStruct((3, groups, 5 * blocks, length), jnp.float32),
                jax.ShapeDtypeStruct((3, groups, blocks, LANES), jnp.int32),
            ],
            in_specs=[pl.BlockSpec(memory_space=pltpu.VMEM)] * 3
            + [pl.BlockSpec(memory_space=pltpu.SMEM)] * 2,
            out_specs=[pl.BlockSpec(memory_space=pl.ANY)] * 2,
            scratch_shapes=[
                pltpu.VMEM((groups, 5 * blocks, length), jnp.float32),
                pltpu.VMEM((groups, blocks, LANES), jnp.int32),
            ]
            + [pltpu.SemaphoreType.DMA((count,)) for count in (copies, copies, 2)],
            compiler_params=pltpu.CompilerParams(collective_id=0, has_side_effects=True),
        )(*own)
        slots = 3 * groups * blocks * length
        return pl.pallas_call(
            lambda *refs: grid_kernel(groups, rows, *refs),
            out_shape=jax.ShapeDtypeStruct((rows, PLANES, 2, NY), jnp.float32),
            in_specs=[
                pl.BlockSpec(memory_space=pl.ANY),
                pl.BlockSpec(memory_space=pltpu.SMEM),
            ],
            out_specs=pl.BlockSpec(memory_space=pl.ANY),
            scratch_shapes=[
                pltpu.VMEM((3, groups, 5 * blocks, length), jnp.float32),
                pltpu.SemaphoreType.DMA,
                pltpu.VMEM((8, slots + 2 * CHUNK), jnp.float32),
                pltpu.VMEM(((PLANES + 1) * 2 * rows, NY), jnp.float32),
                pltpu.VMEM((2 * rows, CHUNK), jnp.bfloat16),
                pltpu.VMEM((CHUNK, NY), jnp.bfloat16),
                pltpu.VMEM((PLANES + 1, 16, CHUNK), jnp.bfloat16),
                pltpu.VMEM((PLANES, rows, 2, NY), jnp.float32),
                pltpu.SMEM((LEVELS + 2,), jnp.int32),
                pltpu.SMEM((LEVELS + 1,), jnp.int32),
                pltpu.SemaphoreType.DMA((PLANES,)),
            ],
            compiler_params=pltpu.CompilerParams(vmem_limit_bytes=60 * 1024 * 1024),
        )(*gathered)

    return jax.shard_map(
        shards,
        mesh=mesh,
        in_specs=(
            P("grp", "slab", None, None, None),
            P("grp", "slab", None, None),
            P("grp", "slab", None, None, None),
            P("grp", "slab", None),
            P("grp", "slab", None),
        ),
        out_specs=P("grp", "slab", None, None),
        check_vma=False,
    )
```
